32 devices in a mesh: scan: 2 (over y), slab: 16 (over z, x, core).
Axes of the slice: x: 2, y: 2, z: 4, core: 2. Of those that a mesh axis runs over, the one named last changes fastest.
Arguments:
- image: float32 [2, 128, 256, 128], P(None, 'slab', 'scan'), parts along dimension 2, may hold values from -6 to 6
- sensitivity: bfloat16 [12, 2, 128, 128, 128], P('scan', None, 'slab'), parts along dimension 0, may hold values from -1.5 to 1.5
- kernel: float32 [256, 256, 256], P(None, 'slab'), may hold values from 0.1 to 4
Outputs:
- normal_image: float32 [2, 128, 256, 128], P(None, 'slab', 'scan'), parts along dimension 2
The draws below stay inside these ranges and needn't reach their ends.
There are 2 independent parts, one for each index of `scan`. The reference program is written for one: setup_inputs(seed, part) draws one part's arguments, and reference() takes and returns one part's arrays. A program takes and returns all parts, laid end to end along the dimension named above; an argument that names none is the same for every part. Nothing has to cross between parts.
All inputs are finite; a program needn't handle non-finite values.
Results may differ from the reference program's by a relative error of at most 0.0024.
Values may be sent and summed in bfloat16 or wider, within the bound.
A program may use at most 128 MiB of HBM per device.

```python
import math
import jax
import jax.numpy as jnp
from jax import lax

NX = 128
NY = 128
NZ = 128
COILS = 6
GX = 256
GY = 256
GZ = 256


def block_levels(key, shape, pieces, smallest, top_value):
    level, own = 1.0, jax.random.fold_in(key, 6)
    for dim, shards_of in pieces:
        draws = jnp.exp(jax.random.uniform(jax.random.fold_in(own, dim), (shards_of,), jnp.float32, smallest / len(pieces), top_value / len(pieces)))
        level = level * jnp.repeat(draws, shape[dim] // shards_of).reshape([-1 if axis == dim else 1 for axis in range(len(shape))])
    return level


def gaussian(own_key, extent, deviation, bound, cuts=(), held_as=jnp.bfloat16):
    values = deviation * jax.random.normal(own_key, extent, jnp.float32)
    if cuts:
        values = values * block_levels(own_key, extent, cuts, -0.22, 0.18)
    return jnp.clip(values, -bound, bound).astype(held_as)


def setup_inputs(seed: int = 0, part: int = 0) -> dict:
    streams_of = jax.random.split(jax.random.key(seed), 4)
    part_splits = jax.random.split(jax.random.fold_in(streams_of[3], part), 4)
    return {
        "image": gaussian(part_splits[0], (2, NX, NY, NZ), 1.0, 6.0, ((1, 16),), jnp.float32),
        "sensitivity": gaussian(part_splits[1], (COILS, 2, NX, NY, NZ), 0.25, 1.5, ((2, 16),)),
        "kernel": jnp.clip(jnp.exp(math.log(4.0) - 3.6888794 * jax.random.uniform(streams_of[2], (GX, GY, GZ), jnp.float32) ** block_levels(streams_of[2], (GX, GY, GZ), ((1, 16),), -0.2, 0.2)), 0.1, 4.0),
    }


smooth_weight = 0.1

def fourier_table(count_out, count_in, length, sign_value):
    row_index = lax.broadcasted_iota(jnp.int32, (count_out, count_in), 0)
    column_index = lax.broadcasted_iota(jnp.int32, (count_out, count_in), 1)
    phases = row_index * column_index % length
    angles = phases.astype(jnp.float32) * (2.0 * math.pi / length)
    factor = 1.0 / math.sqrt(length)
    real_part = jnp.cos(angles) * factor
    imaginary = sign_value * jnp.sin(angles) * factor
    stacked = jnp.stack([jnp.stack([real_part, -imaginary]), jnp.stack([imaginary, real_part])])
    return stacked.astype(jnp.bfloat16)

def transform(matrix, values, pattern):
    return jnp.einsum(pattern, matrix.astype(jnp.float32), values.astype(jnp.float32))

def reference(image, sensitivity, kernel):
    forward_first = fourier_table(GX, NX, GX, -1.0)
    forward_second = fourier_table(GY, NY, GY, -1.0)
    forward_third = fourier_table(GZ, NZ, GZ, -1.0)
    inverse_first = fourier_table(NX, GX, GX, 1.0)
    inverse_second = fourier_table(NY, GY, GY, 1.0)
    inverse_third = fourier_table(NZ, GZ, GZ, 1.0)

    def one_coil(accumulated, coil_maps):
        coil_real = coil_maps[0].astype(jnp.float32)
        coil_imaginary = coil_maps[1].astype(jnp.float32)
        coil_image = jnp.stack([coil_real * image[0] - coil_imaginary * image[1], coil_real * image[1] + coil_imaginary * image[0]]).astype(jnp.bfloat16)
        along_second = transform(forward_second, coil_image, 'pqkj,qajb->pakb').astype(jnp.bfloat16)
        along_third = transform(forward_third, along_second, 'pqkj,qabj->pabk').astype(jnp.bfloat16)
        spectrum = transform(forward_first, along_third, 'pqkj,qjab->pkab')
        filtered = (spectrum * kernel).astype(jnp.bfloat16)
        back_first = transform(inverse_first, filtered, 'pqkj,qjab->pkab').astype(jnp.bfloat16)
        back_third = transform(inverse_third, back_first, 'pqkj,qabj->pabk').astype(jnp.bfloat16)
        coil_result = transform(inverse_second, back_third, 'pqkj,qajb->pakb')
        accumulated = accumulated + jnp.stack([coil_real * coil_result[0] + coil_imaginary * coil_result[1], coil_real * coil_result[1] - coil_imaginary * coil_result[0]])
        return (accumulated, None)
    accumulated = lax.scan(one_coil, jnp.zeros(image.shape, jnp.float32), sensitivity)[0]
    padded = jnp.pad(image, ((0, 0), (1, 1), (1, 1), (1, 1)))
    beside = padded[:, 2:, 1:-1, 1:-1] + padded[:, :-2, 1:-1, 1:-1]
    beside = beside + padded[:, 1:-1, 2:, 1:-1] + padded[:, 1:-1, :-2, 1:-1]
    beside = beside + padded[:, 1:-1, 1:-1, 2:] + padded[:, 1:-1, 1:-1, :-2]
    penalty = 6.0 * image - beside
    return accumulated + smooth_weight * penalty
```

```python
import functools
import math

import jax
import jax.numpy as jnp
import numpy as np
from jax import lax
from jax.experimental import pallas as pl
from jax.experimental.pallas import tpu as pltpu
from jax.sharding import PartitionSpec as P

MESH = pl.DeviceIdType.MESH
smooth_weight = 0.1
F32 = jnp.float32
BF16 = jnp.bfloat16


def factor(count_out, count_in, length, sign_value):
    phases = np.outer(np.arange(count_out), np.arange(count_in)) % length
    angles = phases * (2.0 * math.pi / length)
    scale = 1.0 / math.sqrt(length)
    real, imag = np.cos(angles) * scale, sign_value * np.sin(angles) * scale
    return np.block([[real, -imag], [imag, real]]).astype(jnp.bfloat16)


def dot(a, b):
    return jnp.dot(a, b, preferred_element_type=F32)


def shifted(cells, step, axis):
    count = cells.shape[axis]
    index = lax.broadcasted_iota(jnp.int32, cells.shape, axis)
    edge = 0 if step == 1 else count - 1
    return jnp.where(index == edge, 0.0, pltpu.roll(cells, step % count, axis))


PLANES = 4


def kernel_body(
    n, image, sens, weight, fy, fzt, fx, hx, hzt, hy, out,
    sent, got, home, rows, halo, filt, maps, images, mine, sums, parts, totals,
    send1, recv1, send2, recv2, hsend, hrecv, wsem, msend, mrecv, isend, irecv, tsend, trecv,
):
    me = lax.axis_index("slab")
    coils, _, xs, ny, nz = sens.shape
    gx, gz = fx.shape[0] // 2, weight.shape[1]
    nx, gy = n * xs, fy.shape[0] // 2
    kys = gy // n
    part = kys * xs
    pair = 16 // xs
    last = coils - 1
    cols = n // PLANES
    wide = gy // PLANES
    size = wide * xs
    plane, col = me // cols, lax.rem(me, cols)
    half = plane // 2
    end, mid = 3 * half, 1 + half
    other_mid, other_end = 2 - half, 3 - 3 * half
    hosted = (mid, end, other_mid, other_end)
    is_mid = plane == mid

    columns = [
        pltpu.make_async_copy(weight.at[:, pl.ds(i * 128, 128)], filt.at[i], wsem.at[i])
        for i in range(gz // 128)
    ]
    for copy in columns:
        copy.start()

    barrier = pltpu.get_barrier_semaphore()

    @pl.loop(1, n)
    def _(k):
        pl.semaphore_signal(barrier, inc=1, device_id={"slab": lax.rem(me + k, n)}, device_id_type=MESH)

    pl.semaphore_wait(barrier, n - 1)

    def remote(source, target, send_sem, recv_sem, to):
        return pltpu.make_async_remote_copy(
            src_ref=source, dst_ref=target, send_sem=send_sem, recv_sem=recv_sem,
            device_id={"slab": to}, device_id_type=MESH)

    def halo_copy(p, side):
        edge = xs - 1 if side == 0 else 0
        to = me + 1 if side == 0 else me - 1
        return remote(image.at[p, edge], halo.at[side, p], hsend.at[side, p], hrecv.at[side, p],
                      lax.rem(to + n, n))

    def map_copy(kind, c):
        source = maps.at[0, c] if kind == 2 else sens.at[c]
        to = (mid if kind == 0 else other_mid) * cols + col
        return remote(source, maps.at[kind, c], msend.at[kind, c], mrecv.at[kind, c], to)

    def image_copy(kind):
        source = images.at[0] if kind == 2 else mine
        to = (mid if kind == 0 else other_mid) * cols + col
        return remote(source, images.at[kind], isend.at[kind], irecv.at[kind], to)

    def total_copy(slot):
        landing = 1 if slot == 3 else 0
        return remote(parts.at[slot - 1], totals.at[landing], tsend.at[slot - 1], trecv.at[landing],
                      hosted[slot] * cols + col)

    def act(copy, action):
        if action == "start":
            copy.start()
        elif action == "recv":
            copy.wait_recv()
        else:
            copy.wait_send()

    def around(first, body):
        @pl.loop(first, cols)
        def _(k):
            body(lax.rem(col + k, cols))

    def sent_copy(c, slot, landing, to):
        return remote(sent.at[c, slot], got.at[c, landing], send1.at[c, slot], recv1.at[c, landing], to)

    def back_copy(c, slot, landing, to):
        return remote(got.at[c, slot], home.at[c, landing], send2.at[c, slot], recv2.at[c, landing], to)

    def all_traffic(copy_of, action):
        @pl.loop(1, n)
        def _(k):
            to = lax.rem(me + k, n)
            act(copy_of(last, to, to if action == "recv" else me, to), action)

    def own_plane_out(c, s, action):
        block = (plane if s == 0 else hosted[s]) * cols + col
        around(1, lambda near: act(
            sent_copy(c, s * cols + near, block, plane * cols + near), action))

    def end_plane_out(c, s, action):
        around(0, lambda near: act(
            sent_copy(c, (4 + s) * cols + near, hosted[s] * cols + col, end * cols + near), action))

    def keep_own(c, s):
        got[c, (plane if s == 0 else hosted[s]) * cols + col] = sent[c, s * cols + col]

    def forward_out(c, slots, action):
        for s in slots:
            own_plane_out(c, s, action)
            if s != 1:
                end_plane_out(c, s, action)

    def got_wait(c):
        @pl.when(is_mid)
        def _():
            for s in range(4):
                around(1, lambda near: sent_copy(
                    c, near, hosted[s] * cols + near, plane * cols + near).wait_recv())

        @pl.when(jnp.logical_not(is_mid))
        def _():
            @pl.loop(1, n)
            def _(k):
                block = lax.rem(me + k, n)
                sent_copy(c, 0, block, block).wait_recv()

    def back_out(c, action):
        @pl.when(is_mid)
        def _():
            for s in range(4):
                around(1, lambda near: act(
                    back_copy(c, hosted[s] * cols + near, s * cols + col, plane * cols + near), action))

        @pl.when(jnp.logical_not(is_mid))
        def _():
            for s in (0, 2, 3):
                around(0, lambda near: act(
                    back_copy(c, hosted[s] * cols + near, (4 + s) * cols + col, mid * cols + near), action))
            around(1, lambda near: act(
                back_copy(c, plane * cols + near, col, plane * cols + near), action))

    def back_start(c):
        back_out(c, "start")

        @pl.when(is_mid)
        def _():
            for s in range(4):
                home[c, s * cols + col] = got[c, hosted[s] * cols + col]

        @pl.when(jnp.logical_not(is_mid))
        def _():
            home[c, col] = got[c, me]

    def home_wait(c):
        @pl.when(is_mid)
        def _():
            for s in range(4):
                around(1, lambda near: back_copy(
                    c, 0, s * cols + near, plane * cols + near).wait_recv())
                if s != 1:
                    around(0, lambda near: back_copy(
                        c, 0, (4 + s) * cols + near, end * cols + near).wait_recv())

        @pl.when(jnp.logical_not(is_mid))
        def _():
            around(1, lambda near: back_copy(c, 0, near, plane * cols + near).wait_recv())

    def along_second(table, maps_of, cells_of):
        count = table.shape[0]

        @pl.loop(0, xs // 2)
        def _(h):
            halves = []
            for j in range(2):
                x = 2 * h + j
                cr, ci = maps_of(0, x).astype(F32), maps_of(1, x).astype(F32)
                vr, vi = cells_of(0, x).astype(F32), cells_of(1, x).astype(F32)
                halves.append(jnp.concatenate([cr * vr - ci * vi, cr * vi + ci * vr], axis=0).astype(BF16))
            lines = dot(table, jnp.concatenate(halves, axis=1))
            for j in range(2):
                rows[pl.ds(2 * h + j, count, stride=xs), :] = lines[:, j * nz:(j + 1) * nz]

    def own_maps(c):
        return (lambda p, x: sens[c, p, x]), (lambda p, x: image[p, x])

    def their_maps(c, s):
        return (lambda p, x: maps[s - 1, c, p, x]), (lambda p, x: images[s - 1, p, x])

    def pieces(count, first, place):
        for i in range(count):
            for q in range(2):
                place(i, q, slice((2 * i + q) * size, (2 * i + q + 1) * size), slice(q * part, (q + 1) * part))

    def half_place(i, s):
        return (lax.rem(i + 1 - half, 2) * 4 + s) * cols

    def fill_sent(c, count, start_of):
        def place(i, q, at, to):
            sent[c, pl.ds(start_of(i), cols), to, :] = rows[at, :].reshape(cols, part, nz).astype(BF16)
        pieces(count, 0, place)

    def fill_rows(c, count, start_of):
        def place(i, q, at, to):
            rows[at, :] = home[c, pl.ds(start_of(i), cols), to, :].reshape(size, nz).astype(F32)
        pieces(count, 0, place)

    def half_table():
        return fy[pl.ds(pl.multiple_of(half * 4 * wide, 4 * wide), 4 * wide), :]

    def plane_table():
        return fy[pl.ds(pl.multiple_of(plane * 2 * wide, 2 * wide), 2 * wide), :]

    def forward_half(c, s, sources):
        along_second(half_table(), *sources)
        fill_sent(c, 2, lambda i: half_place(i, s))

    def forward_plane(c, s, sources):
        along_second(plane_table(), *sources)
        fill_sent(c, 1, lambda i: s * cols)

    def forward_own(c):
        @pl.when(is_mid)
        def _():
            forward_half(c, 0, own_maps(c))
            keep_own(c, 0)
            forward_out(c, (0,), "start")

        @pl.when(jnp.logical_not(is_mid))
        def _():
            forward_plane(c, 0, own_maps(c))
            keep_own(c, 0)
            own_plane_out(c, 0, "start")

    def forward_near(c):
        forward_plane(c, 1, their_maps(c, 1))
        keep_own(c, 1)
        forward_out(c, (1,), "start")

    def forward_far(c):
        @pl.loop(2, 4)
        def _(s):
            forward_half(c, s, their_maps(c, s))

        for s in (2, 3):
            keep_own(c, s)
        forward_out(c, (2, 3), "start")

    def forward_last():
        along_second(fy[...], *own_maps(last))
        fill_sent(last, PLANES, lambda i: i * cols)
        all_traffic(sent_copy, "start")
        got[last, me] = sent[last, me]

    def middle(c):
        @pl.loop(0, kys // pair)
        def _(kp):
            base = pl.multiple_of(kp * 16, 16)
            cells = [got[c, :, pl.ds(q * part + base, 16), :].reshape(n * 16, nz) for q in range(2)]
            third = dot(jnp.concatenate(cells, axis=1), fzt[...]).reshape(n, pair, xs, 2 * gz)
            results = []
            for j in range(pair):
                b = third[:, j].reshape(nx, 2 * gz).astype(BF16)
                spectrum = dot(fx[...], jnp.concatenate([b[:, :gz], b[:, gz:]], axis=0))
                k = jnp.concatenate(
                    [filt[i, pl.ds(kp * pair + j, gx, stride=kys), :] for i in range(gz // 128)], axis=1)
                filtered = jnp.concatenate([spectrum[:gx] * k, spectrum[gx:] * k], axis=0).astype(BF16)
                first = dot(hx[...], filtered).astype(BF16)
                results.append(dot(jnp.concatenate([first[:nx], first[nx:]], axis=1), hzt[...]))
            for q in range(2):
                lines = [r[:, q * nz:(q + 1) * nz].reshape(n, 1, xs, nz) for r in results]
                got[c, :, pl.ds(q * part + base, 16), :] = (
                    jnp.concatenate(lines, axis=1).reshape(n, 16, nz).astype(BF16))

    def gather(table, maps_of, acc):
        count = table.shape[1]

        @pl.loop(0, xs // 2)
        def _(h):
            lines = [rows[pl.ds(2 * h + j, count, stride=xs), :] for j in range(2)]
            cells = dot(table, jnp.concatenate(lines, axis=1).astype(BF16))
            for j in range(2):
                x = 2 * h + j
                re, im = cells[:ny, j * nz:(j + 1) * nz], cells[ny:, j * nz:(j + 1) * nz]
                cr, ci = maps_of(0, x).astype(F32), maps_of(1, x).astype(F32)
                acc[0, x] = acc[0, x] + cr * re + ci * im
                acc[1, x] = acc[1, x] + cr * im - ci * re

    def half_back():
        return jnp.concatenate([hy[2 * half], hy[2 * half + 1]], axis=1)

    def inverse(c):
        home_wait(c)

        @pl.when(is_mid)
        def _():
            fill_rows(c, 2, lambda i: half_place(i, 0))
            gather(half_back(), own_maps(c)[0], out)
            fill_rows(c, 1, lambda i: cols)
            gather(hy[plane], their_maps(c, 1)[0], sums.at[0])

            @pl.loop(2, 4)
            def _(s):
                fill_rows(c, 2, lambda i: half_place(i, s))
                gather(half_back(), their_maps(c, s)[0], sums.at[s - 1])

        @pl.when(jnp.logical_not(is_mid))
        def _():
            fill_rows(c, 1, lambda i: 0)
            gather(hy[plane], own_maps(c)[0], out)

    def inverse_last():
        all_traffic(back_copy, "recv")
        fill_rows(last, PLANES, lambda i: i * cols)
        gather(jnp.concatenate([hy[i] for i in range(PLANES)], axis=1), own_maps(last)[0], out)

    def pass_on(c):
        map_copy(1, c).start()
        map_copy(0, c).wait_recv()
        map_copy(2, c).start()

    mine[...] = image[...].astype(BF16)

    @pl.when(is_mid)
    def _():
        image_copy(1).start()
        map_copy(1, 0).start()

    @pl.when(jnp.logical_not(is_mid))
    def _():
        image_copy(0).start()

        @pl.loop(0, last)
        def _(c):
            map_copy(0, c).start()

    @pl.when(me < n - 1)
    def _():
        for p in range(2):
            halo_copy(p, 0).start()

    @pl.when(me > 0)
    def _():
        for p in range(2):
            halo_copy(p, 1).start()

    sums[...] = jnp.zeros_like(sums)
    out[...] = jnp.zeros_like(out)
    forward_own(0)

    @pl.when(is_mid)
    def _():
        image_copy(0).wait_recv()
        image_copy(2).start()
        map_copy(0, 0).wait_recv()
        map_copy(2, 0).start()
        forward_near(0)
        pass_on(1)

    for copy in columns:
        copy.wait()

    @pl.loop(0, coils + 1)
    def _(t):
        @pl.when(jnp.logical_and(is_mid, t + 2 < last))
        def _():
            pass_on(t + 2)

        @pl.when(t + 1 < last)
        def _():
            forward_own(t + 1)

            @pl.when(is_mid)
            def _():
                forward_near(t + 1)

        @pl.when(t == coils - 3)
        def _():
            forward_last()

        @pl.when(jnp.logical_and(is_mid, t < last))
        def _():
            @pl.when(t == 0)
            def _():
                image_copy(1).wait_recv()
                image_copy(2).wait_recv()

            map_copy(1, t).wait_recv()
            map_copy(2, t).wait_recv()
            forward_far(t)

        @pl.when(t > 0)
        def _():
            c = t - 1

            @pl.when(c < last)
            def _():
                got_wait(c)

            @pl.when(c == last)
            def _():
                all_traffic(sent_copy, "recv")

            middle(c)

            @pl.when(c < last)
            def _():
                back_start(c)

            @pl.when(c == last)
            def _():
                all_traffic(back_copy, "start")
                home[last, me] = got[last, me]

        @pl.when(t > 1)
        def _():
            inverse(t - 2)

    @pl.when(is_mid)
    def _():
        parts[...] = sums[...].astype(BF16)
        for s in (2, 3, 1):
            total_copy(s).start()

    @pl.when(me < n - 1)
    def _():
        for p in range(2):
            halo_copy(p, 0).wait_send()
            halo_copy(p, 1).wait_recv()

    @pl.when(me > 0)
    def _():
        for p in range(2):
            halo_copy(p, 1).wait_send()
            halo_copy(p, 0).wait_recv()

    for p in range(2):
        for x in range(xs):
            here = image[p, x]
            if x == 0:
                before = jnp.where(me > 0, halo[0, p], 0.0)
            else:
                before = image[p, x - 1]
            if x == xs - 1:
                after = jnp.where(me < n - 1, halo[1, p], 0.0)
            else:
                after = image[p, x + 1]
            beside = before + after
            for axis in range(2):
                beside = beside + shifted(here, 1, axis) + shifted(here, -1, axis)
            out[p, x] = out[p, x] + smooth_weight * (6.0 * here - beside)

    inverse_last()
    total_copy(2).wait_recv()
    out[...] = out[...] + totals[0].astype(F32)

    @pl.when(jnp.logical_not(is_mid))
    def _():
        total_copy(3).wait_recv()
        out[...] = out[...] + totals[1].astype(F32)

    @pl.loop(0, last)
    def _(c):
        @pl.when(is_mid)
        def _():
            forward_out(c, (0, 1, 2, 3), "send")
            map_copy(1, c).wait_send()
            map_copy(2, c).wait_send()

        @pl.when(jnp.logical_not(is_mid))
        def _():
            own_plane_out(c, 0, "send")
            map_copy(0, c).wait_send()

        back_out(c, "send")

    all_traffic(sent_copy, "send")
    all_traffic(back_copy, "send")

    @pl.when(is_mid)
    def _():
        image_copy(1).wait_send()
        image_copy(2).wait_send()
        for s in (1, 2, 3):
            total_copy(s).wait_send()

    @pl.when(jnp.logical_not(is_mid))
    def _():
        image_copy(0).wait_send()


def fused(n, image, sensitivity, kernel):
    coils, _, xs, ny, nz = sensitivity.shape
    gx, kys, gz = kernel.shape
    nx, gy = n * xs, n * kys
    cols, wide = n // PLANES, gy // PLANES
    block = (2 * kys * xs, nz)
    forward = factor(gy, ny, gy, -1.0).reshape(2, PLANES, wide, 2 * ny)
    backward = factor(ny, gy, gy, 1.0).reshape(2 * ny, 2, PLANES, wide)
    tables = (
        forward.transpose(1, 0, 2, 3).reshape(2 * gy, 2 * ny),
        factor(gz, nz, gz, -1.0).T,
        factor(gx, nx, gx, -1.0),
        factor(nx, gx, gx, 1.0),
        factor(nz, gz, gz, 1.0).T,
        backward.transpose(2, 0, 1, 3).reshape(PLANES, 2 * ny, 2 * wide),
    )
    vmem = pl.BlockSpec(memory_space=pltpu.VMEM)
    dma = pltpu.SemaphoreType.DMA
    slots = 2 * PLANES * cols
    slab = image.shape
    return pl.pallas_call(
        functools.partial(kernel_body, n),
        out_shape=jax.ShapeDtypeStruct(image.shape, F32),
        in_specs=[vmem] * 2 + [pl.BlockSpec(memory_space=pl.ANY)] + [vmem] * 6,
        out_specs=vmem,
        scratch_shapes=[
            pltpu.VMEM((coils, slots, *block), BF16),
            pltpu.VMEM((coils, n, *block), BF16),
            pltpu.VMEM((coils, slots, *block), BF16),
            pltpu.VMEM((2 * gy * xs, nz), F32),
            pltpu.VMEM((2, 2, ny, nz), F32),
            pltpu.VMEM((gz // 128, gx * kys, 128), F32),
            pltpu.VMEM((3, coils - 1, *slab), BF16),
            pltpu.VMEM((3, *slab), BF16),
            pltpu.VMEM(slab, BF16),
            pltpu.VMEM((3, *slab), F32),
            pltpu.VMEM((3, *slab), BF16),
            pltpu.VMEM((2, *slab), BF16),
            dma((coils, slots)), dma((coils, n)), dma((coils, n)), dma((coils, slots)),
            dma((2, 2)), dma((2, 2)), dma((gz // 128,)),
            dma((3, coils)), dma((3, coils)), dma((3,)), dma((3,)), dma((3,)), dma((2,)),
        ],
        compiler_params=pltpu.CompilerParams(
            collective_id=0, has_side_effects=True, vmem_limit_bytes=63 * 2**20),
    )(image, sensitivity, kernel.reshape(gx * kys, gz), *[jnp.asarray(t) for t in tables])


def with_halo(cells, axis, dim):
    count = lax.axis_size(axis)
    head = lax.slice_in_dim(cells, 0, 1, axis=dim)
    tail = lax.slice_in_dim(cells, cells.shape[dim] - 1, cells.shape[dim], axis=dim)
    return jnp.concatenate(
        [
            lax.ppermute(tail, axis, [(i, i + 1) for i in range(count - 1)]),
            cells,
            lax.ppermute(head, axis, [(i + 1, i) for i in range(count - 1)]),
        ],
        axis=dim,
    )


def staged(n, image, sensitivity, kernel):
    coils, _, xs, ny, nz = sensitivity.shape
    gx, kys, gz = kernel.shape
    nx, gy = n * xs, n * kys

    def table(count_out, count_in, length, sign_value):
        both = factor(count_out, count_in, length, sign_value)
        return jnp.asarray(both.reshape(2, count_out, 2, count_in).transpose(0, 2, 1, 3))

    def apply(matrix, values, pattern):
        return jnp.einsum(pattern, matrix, values, preferred_element_type=F32)

    real, imag = sensitivity[:, 0].astype(F32), sensitivity[:, 1].astype(F32)
    images = jnp.stack(
        [real * image[0] - imag * image[1], real * image[1] + imag * image[0]], axis=1).astype(BF16)
    second = apply(table(gy, ny, gy, -1.0), images, "pqkj,cqajb->cpakb").astype(BF16)
    second = lax.all_to_all(second, "slab", split_axis=3, concat_axis=2, tiled=True)
    third = apply(table(gz, nz, gz, -1.0), second, "pqkj,cqabj->cpabk").astype(BF16)
    spectrum = apply(table(gx, nx, gx, -1.0), third, "pqkj,cqjab->cpkab")
    filtered = (spectrum * kernel).astype(BF16)
    first = apply(table(nx, gx, gx, 1.0), filtered, "pqkj,cqjab->cpkab").astype(BF16)
    back = apply(table(nz, gz, gz, 1.0), first, "pqkj,cqabj->cpabk").astype(BF16)
    back = lax.all_to_all(back, "slab", split_axis=2, concat_axis=3, tiled=True)
    cells = apply(table(ny, gy, gy, 1.0), back, "pqkj,cqajb->cpakb")
    summed = jnp.stack([
        jnp.sum(real * cells[:, 0] + imag * cells[:, 1], axis=0),
        jnp.sum(real * cells[:, 1] - imag * cells[:, 0], axis=0)])
    padded = with_halo(image.astype(BF16), "slab", 1).astype(image.dtype)
    beside = padded[:, 2:] + padded[:, :-2]
    wide = jnp.pad(image, ((0, 0), (0, 0), (1, 1), (1, 1)))
    beside = beside + wide[:, :, 2:, 1:-1] + wide[:, :, :-2, 1:-1]
    beside = beside + wide[:, :, 1:-1, 2:] + wide[:, :, 1:-1, :-2]
    return summed + smooth_weight * (6.0 * image - beside)


def solution(mesh):
    n = mesh.shape["slab"]

    def local(image, sensitivity, kernel):
        tiled = sensitivity.shape[2] == 8 and kernel.shape[1] % 2 == 0 and n % PLANES == 0 and sensitivity.shape[0] == 6
        form = fused if tiled else staged
        return form(n, image, sensitivity, kernel)

    return jax.shard_map(
        local,
        mesh=mesh,
        in_specs=(
            P(None, "slab", "scan", None),
            P("scan", None, "slab", None, None),
            P(None, "slab", None),
        ),
        out_specs=P(None, "slab", "scan", None),
        check_vma=False,
    )
```

```python
import functools
import math

import jax
import jax.numpy as jnp
import numpy as np
from jax import lax
from jax.experimental import pallas as pl
from jax.experimental.pallas import tpu as pltpu
from jax.sharding import PartitionSpec as P

MESH = pl.DeviceIdType.MESH
smooth_weight = 0.1
F32 = jnp.float32
BF16 = jnp.bfloat16


def factor(count_out, count_in, length, sign_value):
    phases = np.outer(np.arange(count_out), np.arange(count_in)) % length
    angles = phases * (2.0 * math.pi / length)
    scale = 1.0 / math.sqrt(length)
    real, imag = np.cos(angles) * scale, sign_value * np.sin(angles) * scale
    return np.block([[real, -imag], [imag, real]]).astype(jnp.bfloat16)


def dot(a, b):
    return jnp.dot(a, b, preferred_element_type=F32)


def shifted(cells, step, axis):
    count = cells.shape[axis]
    index = lax.broadcasted_iota(jnp.int32, cells.shape, axis)
    edge = 0 if step == 1 else count - 1
    return jnp.where(index == edge, 0.0, pltpu.roll(cells, step % count, axis))


PLANES = 4
MID_ORDER = (
    ("map", 0), ("mapn", 0), ("img", 0), ("mapn", 3), ("fo", 1), ("map", 1), ("pass", 0), ("imgp", 0),
    ("mapn", 1), ("fl", 0), ("fn", 0), ("pass", 1), ("map", 2), ("fn", 1), ("mapn", 2), ("fo", 0),
    ("imgw", 0), ("ff", 0), ("pass", 2), ("fo", 3), ("fo", 4), ("fo", 2), ("map", 3), ("pass", 3), ("fn", 2),
    ("fn", 3), ("wt", 0), ("mid", 0), ("ff", 1), ("ff", 2), ("mapn", 4), ("mid", 1), ("map", 4), ("pass", 4),
    ("inv", 0), ("ff", 3), ("flf", 0), ("mid", 2), ("ff", 4), ("mid", 3), ("fn", 4), ("mid", 5), ("inv", 2),
    ("inv", 1), ("inv", 3), ("mid", 4), ("inv", 4),
)
END_ORDER = (
    ("mapn", 0), ("img", 0), ("fo", 0), ("mapn", 3), ("fl", 0), ("mapn", 1), ("imgw", 0), ("fn", 1),
    ("fo", 4), ("fo", 3), ("fn", 3), ("mapn", 2), ("fo", 2), ("mapn", 4), ("fo", 1), ("fn", 0), ("wt", 0),
    ("mid", 0), ("mid", 1), ("flf", 0), ("inv", 0), ("fn", 2), ("mid", 3), ("fn", 4), ("mid", 2), ("mid", 4),
    ("mid", 5), ("inv", 1), ("inv", 2), ("inv", 3), ("inv", 4),
)


def kernel_body(
    n, image, sens, weight, fy, fzt, fx, hx, hzt, hy, out,
    sent, got, home, rows, halo, filt, spread, maps, images, mine, sums, parts, totals,
    send1, recv1, send2, recv2, hsend, hrecv, wsem, msend, mrecv, isend, irecv, tsend, trecv,
):
    me = lax.axis_index("slab")
    coils, _, xs, ny, nz = sens.shape
    gx, gz = fx.shape[0] // 2, weight.shape[1]
    nx, gy = n * xs, fy.shape[0] // 2
    kys = gy // n
    part = kys * xs
    pair = 16 // xs
    last = coils - 1
    cols = n // PLANES
    wide = gy // PLANES
    size = wide * xs
    plane, col = me // cols, lax.rem(me, cols)
    half = plane // 2
    end, mid = 3 * half, 1 + half
    other_mid, other_end = 2 - half, 3 - 3 * half
    is_mid = plane == mid
    near_plane = jnp.where(is_mid, end, mid)
    nh = n // 2
    place = lax.rem(me, nh)

    def plane_of(s):
        if isinstance(s, int):
            return (plane, near_plane, other_mid, other_end)[s]
        return jnp.where(s == 2, other_mid, other_end)

    def if_mid(body):
        pl.when(is_mid)(body)

    def if_end(body):
        pl.when(jnp.logical_not(is_mid))(body)

    columns = [
        pltpu.make_async_copy(weight.at[:, pl.ds(i * 128, 128)], filt.at[i], wsem.at[i])
        for i in range(gz // 128)
    ]
    for copy in columns:
        copy.start()

    barrier = pltpu.get_barrier_semaphore()

    @pl.loop(1, n)
    def _(k):
        pl.semaphore_signal(barrier, inc=1, device_id={"slab": lax.rem(me + k, n)}, device_id_type=MESH)

    pl.semaphore_wait(barrier, n - 1)

    def remote(source, target, send_sem, recv_sem, to):
        return pltpu.make_async_remote_copy(
            src_ref=source, dst_ref=target, send_sem=send_sem, recv_sem=recv_sem,
            device_id={"slab": to}, device_id_type=MESH)

    def halo_copy(p, side):
        edge = xs - 1 if side == 0 else 0
        to = me + 1 if side == 0 else me - 1
        return remote(image.at[p, edge], halo.at[side, p], hsend.at[side, p], hrecv.at[side, p],
                      lax.rem(to + n, n))

    def map_copy(s, c):
        source = maps.at[0, c] if isinstance(s, int) and s == 3 else sens.at[c]
        to = (near_plane if isinstance(s, int) and s == 1 else other_mid) * cols + col
        return remote(source, maps.at[s - 1, c], msend.at[s - 1, c], mrecv.at[s - 1, c], to)

    def image_copy(s):
        source = images.at[0] if s == 3 else mine
        to = (near_plane if s == 1 else other_mid) * cols + col
        return remote(source, images.at[s - 1], isend.at[s - 1], irecv.at[s - 1], to)

    def total_copy(s):
        landing = 1 if isinstance(s, int) and s == 1 else 0
        return remote(parts.at[s - 1], totals.at[landing], tsend.at[s - 1], trecv.at[landing],
                      plane_of(s) * cols + col)

    def act(copy, action):
        if action == "start":
            copy.start()
        elif action == "recv":
            copy.wait_recv()
        else:
            copy.wait_send()

    def around(first, body):
        @pl.loop(first, cols)
        def _(k):
            body(lax.rem(col + k, cols))

    def sent_copy(c, slot, landing, to):
        return remote(sent.at[c, slot], got.at[c, landing], send1.at[c, slot], recv1.at[c, landing], to)

    def back_copy(c, slot, landing, to):
        return remote(got.at[c, slot], home.at[c, landing], send2.at[c, slot], recv2.at[c, landing], to)

    def near_half(copy_of, action):
        @pl.loop(1, nh)
        def _(k):
            to = half * nh + lax.rem(place + k, nh)
            act(copy_of(last, to, to if action == "recv" else me, to), action)

    def far_half(copy_of, action):
        @pl.loop(0, nh)
        def _(k):
            to = (1 - half) * nh + lax.rem(place + k, nh)
            act(copy_of(last, to, to if action == "recv" else me, to), action)

    def own_plane_out(c, s, action):
        around(1, lambda near: act(
            sent_copy(c, s * cols + near, plane_of(s) * cols + col, plane * cols + near), action))

    def end_plane_out(c, s, action):
        around(0, lambda near: act(
            sent_copy(c, (2 + s) * cols + near, plane_of(s) * cols + col, end * cols + near), action))

    def keep_own(c, s):
        got[c, plane_of(s) * cols + col] = sent[c, s * cols + col]

    def got_wait(c):
        for s in range(4):
            around(1, lambda near: sent_copy(
                c, near, plane_of(s) * cols + near, plane * cols + near).wait_recv())

        @if_end
        def _():
            for s in (2, 3):
                sent_copy(c, col, plane_of(s) * cols + col, mid * cols + col).wait_recv()

    def back_out(c, action):
        def within(s):
            around(1, lambda near: act(
                back_copy(c, plane_of(s) * cols + near, s * cols + col, plane * cols + near), action))

        def across(s):
            around(0, lambda near: act(
                back_copy(c, plane_of(s) * cols + near, (2 + s) * cols + col, mid * cols + near), action))

        for s in (3, 2):
            if_mid(functools.partial(within, s))
            if_end(functools.partial(across, s))
        for s in (1, 0):
            within(s)

    def back_start(c):
        back_out(c, "start")

        @if_mid
        def _():
            for s in (3, 2):
                home[c, s * cols + col] = got[c, plane_of(s) * cols + col]

        for s in (1, 0):
            home[c, s * cols + col] = got[c, plane_of(s) * cols + col]

    def home_wait(c, s):
        around(1, lambda near: back_copy(c, 0, s * cols + near, plane * cols + near).wait_recv())

    def far_home_wait(c, s):
        home_wait(c, s)
        around(0, lambda near: back_copy(c, 0, (2 + s) * cols + near, end * cols + near).wait_recv())

    def along_second(table, maps_of, cells_of):
        count = table.shape[0]

        @pl.loop(0, xs // 2, unroll=xs // 2)
        def _(h):
            halves = []
            for j in range(2):
                x = 2 * h + j
                cr, ci = maps_of(0, x).astype(F32), maps_of(1, x).astype(F32)
                vr, vi = cells_of(0, x).astype(F32), cells_of(1, x).astype(F32)
                halves.append(jnp.concatenate([cr * vr - ci * vi, cr * vi + ci * vr], axis=0).astype(BF16))
            lines = dot(table, jnp.concatenate(halves, axis=1))
            for j in range(2):
                rows[pl.ds(2 * h + j, count, stride=xs), :] = lines[:, j * nz:(j + 1) * nz]

    def own_maps(c):
        return (lambda p, x: sens[c, p, x]), (lambda p, x: image[p, x])

    def their_maps(c, s):
        return (lambda p, x: maps[s - 1, c, p, x]), (lambda p, x: images[s - 1, p, x])

    def pieces(count, first, place):
        for i in range(count):
            for q in range(2):
                place(i, q, slice((2 * i + q) * size, (2 * i + q + 1) * size), slice(q * part, (q + 1) * part))

    def half_place(i, s):
        return (lax.rem(i + 1 - half, 2) * 2 + s) * cols

    def fill_sent(c, count, start_of):
        def place(i, q, at, to):
            sent[c, pl.ds(start_of(i), cols), to, :] = rows[at, :].reshape(cols, part, nz).astype(BF16)
        pieces(count, 0, place)

    def fill_rows(c, count, start_of):
        def place(i, q, at, to):
            rows[at, :] = home[c, pl.ds(start_of(i), cols), to, :].reshape(size, nz).astype(F32)
        pieces(count, 0, place)

    def half_table():
        return fy[pl.ds(pl.multiple_of(half * 4 * wide, 4 * wide), 4 * wide), :]

    def plane_table():
        return fy[pl.ds(pl.multiple_of(plane * 2 * wide, 2 * wide), 2 * wide), :]

    def forward_half(c, s, sources):
        along_second(half_table(), *sources)
        fill_sent(c, 2, lambda i: half_place(i, s))

    def forward_plane(c, s, sources):
        along_second(plane_table(), *sources)
        fill_sent(c, 1, lambda i: s * cols)

    def forward_own(c):
        forward_plane(c, 0, own_maps(c))
        keep_own(c, 0)
        own_plane_out(c, 0, "start")

    def forward_near(c):
        if_end(lambda: map_copy(1, c).wait_recv())
        forward_plane(c, 1, their_maps(c, 1))
        keep_own(c, 1)
        own_plane_out(c, 1, "start")

    def forward_far(c):
        @pl.loop(2, 4)
        def _(s):
            map_copy(s, c).wait_recv()
            forward_half(c, s, their_maps(c, s))
            keep_own(c, s)
            own_plane_out(c, s, "start")
            end_plane_out(c, s, "start")

    def forward_last(c):
        along_second(fy[...], *own_maps(last))
        fill_sent(last, PLANES, lambda i: i * cols)
        near_half(sent_copy, "start")
        got[last, me] = sent[last, me]

    def forward_last_far(c):
        far_half(sent_copy, "start")

    def middle(c):
        @pl.loop(0, kys // pair)
        def _(kp):
            base = pl.multiple_of(kp * 16, 16)
            cells = [got[c, :, pl.ds(q * part + base, 16), :].reshape(n * 16, nz) for q in range(2)]
            third = dot(jnp.concatenate(cells, axis=1), fzt[...]).reshape(n, pair, xs, 2 * gz)
            halves = [third[:, j].reshape(nx, 2 * gz).astype(BF16) for j in range(pair)]
            spectrum = dot(fx[...], jnp.concatenate(
                [jnp.concatenate([b[:, q * gz:(q + 1) * gz] for b in halves], axis=1) for q in range(2)],
                axis=0))
            k = jnp.concatenate([spread[kp * pair + j] for j in range(pair)], axis=1)
            filtered = jnp.concatenate([spectrum[:gx] * k, spectrum[gx:] * k], axis=0).astype(BF16)
            first = dot(hx[...], filtered).astype(BF16)
            both = dot(jnp.concatenate(
                [jnp.concatenate([first[:nx, j * gz:(j + 1) * gz], first[nx:, j * gz:(j + 1) * gz]], axis=1)
                 for j in range(pair)], axis=0), hzt[...])
            results = [both[j * nx:(j + 1) * nx] for j in range(pair)]
            for q in range(2):
                lines = [r[:, q * nz:(q + 1) * nz].reshape(n, 1, xs, nz) for r in results]
                got[c, :, pl.ds(q * part + base, 16), :] = (
                    jnp.concatenate(lines, axis=1).reshape(n, 16, nz).astype(BF16))

    def gather(table, maps_of, acc):
        count = table.shape[1]

        @pl.loop(0, xs // 2, unroll=xs // 2)
        def _(h):
            lines = [rows[pl.ds(2 * h + j, count, stride=xs), :] for j in range(2)]
            cells = dot(table, jnp.concatenate(lines, axis=1).astype(BF16))
            for j in range(2):
                x = 2 * h + j
                re, im = cells[:ny, j * nz:(j + 1) * nz], cells[ny:, j * nz:(j + 1) * nz]
                cr, ci = maps_of(0, x).astype(F32), maps_of(1, x).astype(F32)
                acc[0, x] = acc[0, x] + cr * re + ci * im
                acc[1, x] = acc[1, x] + cr * im - ci * re

    def half_back():
        return jnp.concatenate([hy[2 * half], hy[2 * half + 1]], axis=1)

    def return_total(c, s):
        @pl.when(c == last - 1)
        def _():
            parts[s - 1] = sums[s - 1].astype(BF16)
            total_copy(s).start()

    def inverse(c):
        @if_mid
        def _():
            @pl.loop(0, 2)
            def _(k):
                s = 3 - k
                far_home_wait(c, s)
                fill_rows(c, 2, lambda i: half_place(i, s))
                gather(half_back(), their_maps(c, s)[0], sums.at[s - 1])
                return_total(c, s)

        home_wait(c, 1)
        fill_rows(c, 1, lambda i: cols)
        gather(hy[plane], their_maps(c, 1)[0], sums.at[0])
        return_total(c, 1)
        home_wait(c, 0)
        fill_rows(c, 1, lambda i: 0)
        gather(hy[plane], own_maps(c)[0], out)

    def inverse_last():
        near_half(back_copy, "recv")
        far_half(back_copy, "recv")
        fill_rows(last, PLANES, lambda i: i * cols)
        gather(jnp.concatenate([hy[i] for i in range(PLANES)], axis=1), own_maps(last)[0], out)

    def pass_map(c):
        map_copy(1, c).wait_recv()
        map_copy(3, c).start()

    def pass_image(c):
        image_copy(1).wait_recv()
        image_copy(3).start()

    def await_image(c):
        if_end(lambda: image_copy(1).wait_recv())

        @if_mid
        def _():
            image_copy(2).wait_recv()
            image_copy(3).wait_recv()

    def start_image(c):
        image_copy(1).start()
        if_mid(lambda: image_copy(2).start())

    def whole_middle(c):
        @pl.when(c < last)
        def _():
            got_wait(c)

        @pl.when(c == last)
        def _():
            near_half(sent_copy, "recv")
            far_half(sent_copy, "recv")

        middle(c)

        @pl.when(c < last)
        def _():
            back_start(c)

        @pl.when(c == last)
        def _():
            far_half(back_copy, "start")
            near_half(back_copy, "start")
            home[last, me] = got[last, me]

    def spread_filter(c):
        for copy in columns:
            copy.wait()

        @pl.loop(0, kys)
        def _(ky):
            for i in range(gz // 128):
                spread[ky, :, i * 128:(i + 1) * 128] = filt[i, pl.ds(ky, gx, stride=kys), :]

    steps = {
        "wt": spread_filter,
        "img": start_image, "imgp": pass_image, "imgw": await_image,
        "map": lambda c: map_copy(2, c).start(), "mapn": lambda c: map_copy(1, c).start(),
        "pass": pass_map, "fo": forward_own, "fn": forward_near, "ff": forward_far,
        "fl": forward_last, "flf": forward_last_far, "mid": whole_middle, "inv": inverse,
    }

    mine[...] = image[...].astype(BF16)

    @pl.when(me < n - 1)
    def _():
        for p in range(2):
            halo_copy(p, 0).start()

    @pl.when(me > 0)
    def _():
        for p in range(2):
            halo_copy(p, 1).start()

    sums[...] = jnp.zeros_like(sums)
    out[...] = jnp.zeros_like(out)
    @pl.loop(0, max(len(MID_ORDER), len(END_ORDER)))
    def _(t):
        for name, body in steps.items():
            chosen = [
                sum(jnp.where(t == i, c + 1, 0) for i, (other, c) in enumerate(order) if other == name)
                for order in (MID_ORDER, END_ORDER)
            ]
            code = jnp.where(is_mid, *chosen)
            pl.when(code > 0)(functools.partial(body, code - 1))

    @pl.when(me < n - 1)
    def _():
        for p in range(2):
            halo_copy(p, 0).wait_send()
            halo_copy(p, 1).wait_recv()

    @pl.when(me > 0)
    def _():
        for p in range(2):
            halo_copy(p, 1).wait_send()
            halo_copy(p, 0).wait_recv()

    for p in range(2):
        for x in range(xs):
            here = image[p, x]
            if x == 0:
                before = jnp.where(me > 0, halo[0, p], 0.0)
            else:
                before = image[p, x - 1]
            if x == xs - 1:
                after = jnp.where(me < n - 1, halo[1, p], 0.0)
            else:
                after = image[p, x + 1]
            beside = before + after
            for axis in range(2):
                beside = beside + shifted(here, 1, axis) + shifted(here, -1, axis)
            out[p, x] = out[p, x] + smooth_weight * (6.0 * here - beside)

    inverse_last()
    total_copy(1).wait_recv()
    total_copy(2).wait_recv()
    out[...] = out[...] + totals[0].astype(F32) + totals[1].astype(F32)

    @pl.loop(0, last)
    def _(c):
        for s in range(2):
            own_plane_out(c, s, "send")
        map_copy(1, c).wait_send()

        @if_mid
        def _():
            for s in (2, 3):
                own_plane_out(c, s, "send")
                end_plane_out(c, s, "send")
                map_copy(s, c).wait_send()

        back_out(c, "send")

    for copy_of in (sent_copy, back_copy):
        near_half(copy_of, "send")
        far_half(copy_of, "send")
    image_copy(1).wait_send()
    total_copy(1).wait_send()

    @if_mid
    def _():
        for s in (2, 3):
            image_copy(s).wait_send()
            total_copy(s).wait_send()


def fused(n, image, sensitivity, kernel):
    coils, _, xs, ny, nz = sensitivity.shape
    gx, kys, gz = kernel.shape
    nx, gy = n * xs, n * kys
    cols, wide = n // PLANES, gy // PLANES
    block = (2 * kys * xs, nz)
    forward = factor(gy, ny, gy, -1.0).reshape(2, PLANES, wide, 2 * ny)
    backward = factor(ny, gy, gy, 1.0).reshape(2 * ny, 2, PLANES, wide)
    tables = (
        forward.transpose(1, 0, 2, 3).reshape(2 * gy, 2 * ny),
        factor(gz, nz, gz, -1.0).T,
        factor(gx, nx, gx, -1.0),
        factor(nx, gx, gx, 1.0),
        factor(nz, gz, gz, 1.0).T,
        backward.transpose(2, 0, 1, 3).reshape(PLANES, 2 * ny, 2 * wide),
    )
    vmem = pl.BlockSpec(memory_space=pltpu.VMEM)
    dma = pltpu.SemaphoreType.DMA
    slots = (PLANES + 2) * cols
    slab = image.shape
    return pl.pallas_call(
        functools.partial(kernel_body, n),
        out_shape=jax.ShapeDtypeStruct(image.shape, F32),
        in_specs=[vmem] * 2 + [pl.BlockSpec(memory_space=pl.ANY)] + [vmem] * 6,
        out_specs=vmem,
        scratch_shapes=[
            pltpu.VMEM((coils, slots, *block), BF16),
            pltpu.VMEM((coils, n, *block), BF16),
            pltpu.VMEM((coils, slots, *block), BF16),
            pltpu.VMEM((2 * gy * xs, nz), F32),
            pltpu.VMEM((2, 2, ny, nz), F32),
            pltpu.VMEM((gz // 128, gx * kys, 128), F32),
            pltpu.VMEM((kys, gx, gz), F32),
            pltpu.VMEM((3, coils - 1, *slab), BF16),
            pltpu.VMEM((3, *slab), BF16),
            pltpu.VMEM(slab, BF16),
            pltpu.VMEM((3, *slab), F32),
            pltpu.VMEM((3, *slab), BF16),
            pltpu.VMEM((2, *slab), BF16),
            dma((coils, slots)), dma((coils, n)), dma((coils, n)), dma((coils, slots)),
            dma((2, 2)), dma((2, 2)), dma((gz // 128,)),
            dma((3, coils)), dma((3, coils)), dma((3,)), dma((3,)), dma((3,)), dma((2,)),
        ],
        compiler_params=pltpu.CompilerParams(
            collective_id=0, has_side_effects=True, vmem_limit_bytes=63 * 2**20),
    )(image, sensitivity, kernel.reshape(gx * kys, gz), *[jnp.asarray(t) for t in tables])


def with_halo(cells, axis, dim):
    count = lax.axis_size(axis)
    head = lax.slice_in_dim(cells, 0, 1, axis=dim)
    tail = lax.slice_in_dim(cells, cells.shape[dim] - 1, cells.shape[dim], axis=dim)
    return jnp.concatenate(
        [
            lax.ppermute(tail, axis, [(i, i + 1) for i in range(count - 1)]),
            cells,
            lax.ppermute(head, axis, [(i + 1, i) for i in range(count - 1)]),
        ],
        axis=dim,
    )


def staged(n, image, sensitivity, kernel):
    coils, _, xs, ny, nz = sensitivity.shape
    gx, kys, gz = kernel.shape
    nx, gy = n * xs, n * kys

    def table(count_out, count_in, length, sign_value):
        both = factor(count_out, count_in, length, sign_value)
        return jnp.asarray(both.reshape(2, count_out, 2, count_in).transpose(0, 2, 1, 3))

    def apply(matrix, values, pattern):
        return jnp.einsum(pattern, matrix, values, preferred_element_type=F32)

    real, imag = sensitivity[:, 0].astype(F32), sensitivity[:, 1].astype(F32)
    images = jnp.stack(
        [real * image[0] - imag * image[1], real * image[1] + imag * image[0]], axis=1).astype(BF16)
    second = apply(table(gy, ny, gy, -1.0), images, "pqkj,cqajb->cpakb").astype(BF16)
    second = lax.all_to_all(second, "slab", split_axis=3, concat_axis=2, tiled=True)
    third = apply(table(gz, nz, gz, -1.0), second, "pqkj,cqabj->cpabk").astype(BF16)
    spectrum = apply(table(gx, nx, gx, -1.0), third, "pqkj,cqjab->cpkab")
    filtered = (spectrum * kernel).astype(BF16)
    first = apply(table(nx, gx, gx, 1.0), filtered, "pqkj,cqjab->cpkab").astype(BF16)
    back = apply(table(nz, gz, gz, 1.0), first, "pqkj,cqabj->cpabk").astype(BF16)
    back = lax.all_to_all(back, "slab", split_axis=2, concat_axis=3, tiled=True)
    cells = apply(table(ny, gy, gy, 1.0), back, "pqkj,cqajb->cpakb")
    summed = jnp.stack([
        jnp.sum(real * cells[:, 0] + imag * cells[:, 1], axis=0),
        jnp.sum(real * cells[:, 1] - imag * cells[:, 0], axis=0)])
    padded = with_halo(image.astype(BF16), "slab", 1).astype(image.dtype)
    beside = padded[:, 2:] + padded[:, :-2]
    wide = jnp.pad(image, ((0, 0), (0, 0), (1, 1), (1, 1)))
    beside = beside + wide[:, :, 2:, 1:-1] + wide[:, :, :-2, 1:-1]
    beside = beside + wide[:, :, 1:-1, 2:] + wide[:, :, 1:-1, :-2]
    return summed + smooth_weight * (6.0 * image - beside)


def solution(mesh):
    n = mesh.shape["slab"]

    def local(image, sensitivity, kernel):
        tiled = sensitivity.shape[2] == 8 and kernel.shape[1] % 2 == 0 and n % PLANES == 0 and sensitivity.shape[0] == 6
        form = fused if tiled else staged
        return form(n, image, sensitivity, kernel)

    return jax.shard_map(
        local,
        mesh=mesh,
        in_specs=(
            P(None, "slab", "scan", None),
            P("scan", None, "slab", None, None),
            P(None, "slab", None),
        ),
        out_specs=P(None, "slab", "scan", None),
        check_vma=False,
    )
```

```python
import functools
import math

import jax
import jax.numpy as jnp
import numpy as np
from jax import lax
from jax.experimental import pallas as pl
from jax.experimental.pallas import tpu as pltpu
from jax.sharding import PartitionSpec as P

MESH = pl.DeviceIdType.MESH
smooth_weight = 0.1
F32 = jnp.float32
BF16 = jnp.bfloat16


def factor(count_out, count_in, length, sign_value):
    phases = np.outer(np.arange(count_out), np.arange(count_in)) % length
    angles = phases * (2.0 * math.pi / length)
    scale = 1.0 / math.sqrt(length)
    real, imag = np.cos(angles) * scale, sign_value * np.sin(angles) * scale
    return np.block([[real, -imag], [imag, real]]).astype(jnp.bfloat16)


def dot(a, b):
    return jnp.dot(a, b, preferred_element_type=F32)


def shifted(cells, step, axis):
    count = cells.shape[axis]
    index = lax.broadcasted_iota(jnp.int32, cells.shape, axis)
    edge = 0 if step == 1 else count - 1
    return jnp.where(index == edge, 0.0, pltpu.roll(cells, step % count, axis))


PLANES = 4
MID_ORDER = (
    ("map", 0), ("img", 0), ("mapn", 0), ("fo", 0), ("fo", 1), ("fo", 2), ("fo", 3), ("fo", 4), ("mapn", 1),
    ("map", 1), ("mapn", 2), ("pass", 0), ("imgp", 0), ("fn", 0), ("pass", 1), ("fn", 1), ("map", 2),
    ("mapn", 3), ("imgw", 0), ("ff", 0), ("fl", 0), ("pass", 2), ("fn", 2), ("map", 3), ("mapn", 4),
    ("ff", 1), ("pass", 3), ("fn", 3), ("wt", 0), ("mid", 0), ("map", 4), ("ff", 2), ("mid", 1), ("pass", 4),
    ("fn", 4), ("inv", 0), ("ff", 3), ("mid", 2), ("flf", 0), ("ff", 4), ("mid", 3), ("mid", 4), ("inv", 1),
    ("mid", 5), ("inv", 2), ("inv", 3), ("inv", 4),
)
END_ORDER = (
    ("img", 0), ("mapn", 0), ("fo", 0), ("fo", 1), ("mapn", 1), ("fo", 2), ("fo", 3), ("fo", 4), ("mapn", 2),
    ("mapn", 3), ("mapn", 4), ("fl", 0), ("imgw", 0), ("fn", 0), ("fn", 1), ("fn", 2), ("fn", 3), ("wt", 0),
    ("mid", 0), ("fn", 4), ("mid", 1), ("flf", 0), ("inv", 0), ("mid", 2), ("inv", 1), ("mid", 3), ("mid", 4),
    ("mid", 5), ("inv", 2), ("inv", 3), ("inv", 4),
)


def kernel_body(
    n, image_in, sens_in, weight, *rest,
):
    names, rest = rest[:6], rest[6:]
    (out, image, sens, fy, fzt, fx, hx, hzt, hy, load, sent, got, home, rows, halo, filt, spread, maps, images, mine, sums, parts, totals,
    send1, recv1, send2, recv2, hsend, hrecv, wsem, msend, mrecv, isend, irecv, tsend, trecv) = rest
    me = lax.axis_index("slab")
    coils, _, xs, ny, nz = sens.shape
    gx, gz = fx.shape[0] // 2, weight.shape[1]
    nx, gy = n * xs, fy.shape[0] // 2
    kys = gy // n
    part = kys * xs
    pair = 16 // xs
    last = coils - 1
    cols = n // PLANES
    wide = gy // PLANES
    size = wide * xs
    plane, col = me // cols, lax.rem(me, cols)
    half = plane // 2
    end, mid = 3 * half, 1 + half
    other_mid, other_end = 2 - half, 3 - 3 * half
    is_mid = plane == mid
    near_plane = jnp.where(is_mid, end, mid)
    nh = n // 2
    place = lax.rem(me, nh)

    def plane_of(s):
        if isinstance(s, int):
            return (plane, near_plane, other_mid, other_end)[s]
        return jnp.where(s == 2, other_mid, other_end)

    def if_mid(body):
        pl.when(is_mid)(body)

    def if_end(body):
        pl.when(jnp.logical_not(is_mid))(body)

    loads = [
        pltpu.make_async_copy(source, target, load.at[i])
        for i, (source, target) in enumerate(zip(
            (sens_in, image_in, *names), (sens, image, fy, fzt, fx, hx, hzt, hy)))
    ]
    for copy in loads:
        copy.start()

    columns = [
        pltpu.make_async_copy(weight.at[:, pl.ds(i * 128, 128)], filt.at[i], wsem.at[i])
        for i in range(gz // 128)
    ]
    for copy in columns:
        copy.start()

    barrier = pltpu.get_barrier_semaphore()

    @pl.loop(1, n)
    def _(k):
        pl.semaphore_signal(barrier, inc=1, device_id={"slab": lax.rem(me + k, n)}, device_id_type=MESH)

    pl.semaphore_wait(barrier, n - 1)

    def remote(source, target, send_sem, recv_sem, to):
        return pltpu.make_async_remote_copy(
            src_ref=source, dst_ref=target, send_sem=send_sem, recv_sem=recv_sem,
            device_id={"slab": to}, device_id_type=MESH)

    def halo_copy(p, side):
        edge = xs - 1 if side == 0 else 0
        to = me + 1 if side == 0 else me - 1
        return remote(image.at[p, edge], halo.at[side, p], hsend.at[side, p], hrecv.at[side, p],
                      lax.rem(to + n, n))

    def map_copy(s, c):
        source = maps.at[0, c] if isinstance(s, int) and s == 3 else sens.at[c]
        to = (near_plane if isinstance(s, int) and s == 1 else other_mid) * cols + col
        return remote(source, maps.at[s - 1, c], msend.at[s - 1, c], mrecv.at[s - 1, c], to)

    def image_copy(s):
        source = images.at[0] if s == 3 else mine
        to = (near_plane if s == 1 else other_mid) * cols + col
        return remote(source, images.at[s - 1], isend.at[s - 1], irecv.at[s - 1], to)

    def total_copy(s):
        landing = 1 if isinstance(s, int) and s == 1 else 0
        return remote(parts.at[s - 1], totals.at[landing], tsend.at[s - 1], trecv.at[landing],
                      plane_of(s) * cols + col)

    def act(copy, action):
        if action == "start":
            copy.start()
        elif action == "recv":
            copy.wait_recv()
        else:
            copy.wait_send()

    def around(first, body):
        @pl.loop(first, cols)
        def _(k):
            body(lax.rem(col + k, cols))

    def sent_copy(c, slot, landing, to):
        return remote(sent.at[c, slot], got.at[c, landing], send1.at[c, slot], recv1.at[c, landing], to)

    def back_copy(c, slot, landing, to):
        return remote(got.at[c, slot], home.at[c, landing], send2.at[c, slot], recv2.at[c, landing], to)

    def near_half(copy_of, action):
        @pl.loop(1, nh)
        def _(k):
            to = half * nh + lax.rem(place + k, nh)
            act(copy_of(last, to, to if action == "recv" else me, to), action)

    def far_half(copy_of, action):
        @pl.loop(0, nh)
        def _(k):
            to = (1 - half) * nh + lax.rem(place + k, nh)
            act(copy_of(last, to, to if action == "recv" else me, to), action)

    def own_plane_out(c, s, action):
        around(1, lambda near: act(
            sent_copy(c, s * cols + near, plane_of(s) * cols + col, plane * cols + near), action))

    def end_plane_out(c, s, action):
        around(0, lambda near: act(
            sent_copy(c, (2 + s) * cols + near, plane_of(s) * cols + col, end * cols + near), action))

    def keep_own(c, s):
        got[c, plane_of(s) * cols + col] = sent[c, s * cols + col]

    def got_wait(c):
        for s in range(4):
            around(1, lambda near: sent_copy(
                c, near, plane_of(s) * cols + near, plane * cols + near).wait_recv())

        @if_end
        def _():
            for s in (2, 3):
                sent_copy(c, col, plane_of(s) * cols + col, mid * cols + col).wait_recv()

    def back_out(c, action):
        def within(s):
            around(1, lambda near: act(
                back_copy(c, plane_of(s) * cols + near, s * cols + col, plane * cols + near), action))

        def across(s):
            around(0, lambda near: act(
                back_copy(c, plane_of(s) * cols + near, (2 + s) * cols + col, mid * cols + near), action))

        for s in (3, 2):
            if_mid(functools.partial(within, s))
            if_end(functools.partial(across, s))
        for s in (1, 0):
            within(s)

    def back_start(c):
        back_out(c, "start")

        @if_mid
        def _():
            for s in (3, 2):
                home[c, s * cols + col] = got[c, plane_of(s) * cols + col]

        for s in (1, 0):
            home[c, s * cols + col] = got[c, plane_of(s) * cols + col]

    def home_wait(c, s):
        around(1, lambda near: back_copy(c, 0, s * cols + near, plane * cols + near).wait_recv())

    def far_home_wait(c, s):
        home_wait(c, s)
        around(0, lambda near: back_copy(c, 0, (2 + s) * cols + near, end * cols + near).wait_recv())

    def along_second(table, maps_of, cells_of):
        count = table.shape[0]

        @pl.loop(0, xs // 2, unroll=xs // 2)
        def _(h):
            halves = []
            for j in range(2):
                x = 2 * h + j
                cr, ci = maps_of(0, x).astype(F32), maps_of(1, x).astype(F32)
                vr, vi = cells_of(0, x).astype(F32), cells_of(1, x).astype(F32)
                halves.append(jnp.concatenate([cr * vr - ci * vi, cr * vi + ci * vr], axis=0).astype(BF16))
            lines = dot(table, jnp.concatenate(halves, axis=1))
            for j in range(2):
                rows[pl.ds(2 * h + j, count, stride=xs), :] = lines[:, j * nz:(j + 1) * nz]

    def own_maps(c):
        return (lambda p, x: sens[c, p, x]), (lambda p, x: image[p, x])

    def their_maps(c, s):
        return (lambda p, x: maps[s - 1, c, p, x]), (lambda p, x: images[s - 1, p, x])

    def pieces(count, first, place):
        for i in range(count):
            for q in range(2):
                place(i, q, slice((2 * i + q) * size, (2 * i + q + 1) * size), slice(q * part, (q + 1) * part))

    def half_place(i, s):
        return (lax.rem(i + 1 - half, 2) * 2 + s) * cols

    def fill_sent(c, count, start_of):
        def place(i, q, at, to):
            sent[c, pl.ds(start_of(i), cols), to, :] = rows[at, :].reshape(cols, part, nz).astype(BF16)
        pieces(count, 0, place)

    def fill_rows(c, count, start_of):
        def place(i, q, at, to):
            rows[at, :] = home[c, pl.ds(start_of(i), cols), to, :].reshape(size, nz).astype(F32)
        pieces(count, 0, place)

    def half_table():
        return fy[pl.ds(pl.multiple_of(half * 4 * wide, 4 * wide), 4 * wide), :]

    def plane_table():
        return fy[pl.ds(pl.multiple_of(plane * 2 * wide, 2 * wide), 2 * wide), :]

    def forward_half(c, s, sources):
        along_second(half_table(), *sources)
        fill_sent(c, 2, lambda i: half_place(i, s))

    def forward_plane(c, s, sources):
        along_second(plane_table(), *sources)
        fill_sent(c, 1, lambda i: s * cols)

    def forward_own(c):
        forward_plane(c, 0, own_maps(c))
        keep_own(c, 0)
        own_plane_out(c, 0, "start")

    def forward_near(c):
        if_end(lambda: map_copy(1, c).wait_recv())
        forward_plane(c, 1, their_maps(c, 1))
        keep_own(c, 1)
        own_plane_out(c, 1, "start")

    def forward_far(c):
        @pl.loop(2, 4)
        def _(s):
            map_copy(s, c).wait_recv()
            forward_half(c, s, their_maps(c, s))
            keep_own(c, s)
            own_plane_out(c, s, "start")
            end_plane_out(c, s, "start")

    def forward_last(c):
        along_second(fy[...], *own_maps(last))
        fill_sent(last, PLANES, lambda i: i * cols)
        near_half(sent_copy, "start")
        got[last, me] = sent[last, me]

    def forward_last_far(c):
        far_half(sent_copy, "start")

    def middle(c):
        @pl.loop(0, kys // pair)
        def _(kp):
            base = pl.multiple_of(kp * 16, 16)
            cells = [got[c, :, pl.ds(q * part + base, 16), :].reshape(n * 16, nz) for q in range(2)]
            third = dot(jnp.concatenate(cells, axis=1), fzt[...]).reshape(n, pair, xs, 2 * gz)
            halves = [third[:, j].reshape(nx, 2 * gz).astype(BF16) for j in range(pair)]
            spectrum = dot(fx[...], jnp.concatenate(
                [jnp.concatenate([b[:, q * gz:(q + 1) * gz] for b in halves], axis=1) for q in range(2)],
                axis=0))
            k = jnp.concatenate([spread[kp * pair + j] for j in range(pair)], axis=1)
            filtered = jnp.concatenate([spectrum[:gx] * k, spectrum[gx:] * k], axis=0).astype(BF16)
            first = dot(hx[...], filtered).astype(BF16)
            both = dot(jnp.concatenate(
                [jnp.concatenate([first[:nx, j * gz:(j + 1) * gz], first[nx:, j * gz:(j + 1) * gz]], axis=1)
                 for j in range(pair)], axis=0), hzt[...])
            results = [both[j * nx:(j + 1) * nx] for j in range(pair)]
            for q in range(2):
                lines = [r[:, q * nz:(q + 1) * nz].reshape(n, 1, xs, nz) for r in results]
                got[c, :, pl.ds(q * part + base, 16), :] = (
                    jnp.concatenate(lines, axis=1).reshape(n, 16, nz).astype(BF16))

    def gather(table, maps_of, acc):
        count = table.shape[1]

        @pl.loop(0, xs // 2, unroll=xs // 2)
        def _(h):
            lines = [rows[pl.ds(2 * h + j, count, stride=xs), :] for j in range(2)]
            cells = dot(table, jnp.concatenate(lines, axis=1).astype(BF16))
            for j in range(2):
                x = 2 * h + j
                re, im = cells[:ny, j * nz:(j + 1) * nz], cells[ny:, j * nz:(j + 1) * nz]
                cr, ci = maps_of(0, x).astype(F32), maps_of(1, x).astype(F32)
                acc[0, x] = acc[0, x] + cr * re + ci * im
                acc[1, x] = acc[1, x] + cr * im - ci * re

    def half_back():
        return jnp.concatenate([hy[2 * half], hy[2 * half + 1]], axis=1)

    def return_total(c, s):
        @pl.when(c == last - 1)
        def _():
            parts[s - 1] = sums[s - 1].astype(BF16)
            total_copy(s).start()

    def inverse(c):
        @if_mid
        def _():
            @pl.loop(0, 2)
            def _(k):
                s = 3 - k
                far_home_wait(c, s)
                fill_rows(c, 2, lambda i: half_place(i, s))
                gather(half_back(), their_maps(c, s)[0], sums.at[s - 1])
                return_total(c, s)

        home_wait(c, 1)
        fill_rows(c, 1, lambda i: cols)
        gather(hy[plane], their_maps(c, 1)[0], sums.at[0])
        return_total(c, 1)
        home_wait(c, 0)
        fill_rows(c, 1, lambda i: 0)
        gather(hy[plane], own_maps(c)[0], out)

    def inverse_last():
        near_half(back_copy, "recv")
        far_half(back_copy, "recv")
        fill_rows(last, PLANES, lambda i: i * cols)
        gather(jnp.concatenate([hy[i] for i in range(PLANES)], axis=1), own_maps(last)[0], out)

    def pass_map(c):
        map_copy(1, c).wait_recv()
        map_copy(3, c).start()

    def pass_image(c):
        image_copy(1).wait_recv()
        image_copy(3).start()

    def await_image(c):
        if_end(lambda: image_copy(1).wait_recv())

        @if_mid
        def _():
            image_copy(2).wait_recv()
            image_copy(3).wait_recv()

    def start_image(c):
        image_copy(1).start()
        if_mid(lambda: image_copy(2).start())

    def whole_middle(c):
        @pl.when(c < last)
        def _():
            got_wait(c)

        @pl.when(c == last)
        def _():
            near_half(sent_copy, "recv")
            far_half(sent_copy, "recv")

        middle(c)

        @pl.when(c < last)
        def _():
            back_start(c)

        @pl.when(c == last)
        def _():
            far_half(back_copy, "start")
            near_half(back_copy, "start")
            home[last, me] = got[last, me]

    def spread_filter(c):
        @pl.when(me < n - 1)
        def _():
            for p in range(2):
                halo_copy(p, 0).start()

        @pl.when(me > 0)
        def _():
            for p in range(2):
                halo_copy(p, 1).start()

        sums[...] = jnp.zeros_like(sums)
        out[...] = jnp.zeros_like(out)

        for copy in columns:
            copy.wait()

        @pl.loop(0, kys)
        def _(ky):
            for i in range(gz // 128):
                spread[ky, :, i * 128:(i + 1) * 128] = filt[i, pl.ds(ky, gx, stride=kys), :]

    steps = {
        "wt": spread_filter,
        "img": start_image, "imgp": pass_image, "imgw": await_image,
        "map": lambda c: map_copy(2, c).start(), "mapn": lambda c: map_copy(1, c).start(),
        "pass": pass_map, "fo": forward_own, "fn": forward_near, "ff": forward_far,
        "fl": forward_last, "flf": forward_last_far, "mid": whole_middle, "inv": inverse,
    }

    for copy in loads:
        copy.wait()

    mine[...] = image[...].astype(BF16)

    @pl.loop(0, max(len(MID_ORDER), len(END_ORDER)))
    def _(t):
        for name, body in steps.items():
            chosen = [
                sum(jnp.where(t == i, c + 1, 0) for i, (other, c) in enumerate(order) if other == name)
                for order in (MID_ORDER, END_ORDER)
            ]
            code = jnp.where(is_mid, *chosen)
            pl.when(code > 0)(functools.partial(body, code - 1))

    @pl.when(me < n - 1)
    def _():
        for p in range(2):
            halo_copy(p, 0).wait_send()
            halo_copy(p, 1).wait_recv()

    @pl.when(me > 0)
    def _():
        for p in range(2):
            halo_copy(p, 1).wait_send()
            halo_copy(p, 0).wait_recv()

    for p in range(2):
        for x in range(xs):
            here = image[p, x]
            if x == 0:
                before = jnp.where(me > 0, halo[0, p], 0.0)
            else:
                before = image[p, x - 1]
            if x == xs - 1:
                after = jnp.where(me < n - 1, halo[1, p], 0.0)
            else:
                after = image[p, x + 1]
            beside = before + after
            for axis in range(2):
                beside = beside + shifted(here, 1, axis) + shifted(here, -1, axis)
            out[p, x] = out[p, x] + smooth_weight * (6.0 * here - beside)

    inverse_last()
    total_copy(1).wait_recv()
    total_copy(2).wait_recv()
    out[...] = out[...] + totals[0].astype(F32) + totals[1].astype(F32)

    @pl.loop(0, last)
    def _(c):
        for s in range(2):
            own_plane_out(c, s, "send")
        map_copy(1, c).wait_send()

        @if_mid
        def _():
            for s in (2, 3):
                own_plane_out(c, s, "send")
                end_plane_out(c, s, "send")
                map_copy(s, c).wait_send()

        back_out(c, "send")

    for copy_of in (sent_copy, back_copy):
        near_half(copy_of, "send")
        far_half(copy_of, "send")
    image_copy(1).wait_send()
    total_copy(1).wait_send()

    @if_mid
    def _():
        for s in (2, 3):
            image_copy(s).wait_send()
            total_copy(s).wait_send()


def fused(n, image, sensitivity, kernel):
    coils, _, xs, ny, nz = sensitivity.shape
    gx, kys, gz = kernel.shape
    nx, gy = n * xs, n * kys
    cols, wide = n // PLANES, gy // PLANES
    block = (2 * kys * xs, nz)
    forward = factor(gy, ny, gy, -1.0).reshape(2, PLANES, wide, 2 * ny)
    backward = factor(ny, gy, gy, 1.0).reshape(2 * ny, 2, PLANES, wide)
    tables = (
        forward.transpose(1, 0, 2, 3).reshape(2 * gy, 2 * ny),
        factor(gz, nz, gz, -1.0).T,
        factor(gx, nx, gx, -1.0),
        factor(nx, gx, gx, 1.0),
        factor(nz, gz, gz, 1.0).T,
        backward.transpose(2, 0, 1, 3).reshape(PLANES, 2 * ny, 2 * wide),
    )
    vmem = pl.BlockSpec(memory_space=pltpu.VMEM)
    dma = pltpu.SemaphoreType.DMA
    slots = (PLANES + 2) * cols
    slab = image.shape
    return pl.pallas_call(
        functools.partial(kernel_body, n),
        out_shape=jax.ShapeDtypeStruct(image.shape, F32),
        in_specs=[pl.BlockSpec(memory_space=pl.ANY)] * 9,
        out_specs=vmem,
        scratch_shapes=[
            pltpu.VMEM(image.shape, F32),
            pltpu.VMEM(sensitivity.shape, BF16),
            *[pltpu.VMEM(t.shape, BF16) for t in tables],
            dma((8,)),
            pltpu.VMEM((coils, slots, *block), BF16),
            pltpu.VMEM((coils, n, *block), BF16),
            pltpu.VMEM((coils, slots, *block), BF16),
            pltpu.VMEM((2 * gy * xs, nz), F32),
            pltpu.VMEM((2, 2, ny, nz), F32),
            pltpu.VMEM((gz // 128, gx * kys, 128), F32),
            pltpu.VMEM((kys, gx, gz), F32),
            pltpu.VMEM((3, coils - 1, *slab), BF16),
            pltpu.VMEM((3, *slab), BF16),
            pltpu.VMEM(slab, BF16),
            pltpu.VMEM((3, *slab), F32),
            pltpu.VMEM((3, *slab), BF16),
            pltpu.VMEM((2, *slab), BF16),
            dma((coils, slots)), dma((coils, n)), dma((coils, n)), dma((coils, slots)),
            dma((2, 2)), dma((2, 2)), dma((gz // 128,)),
            dma((3, coils)), dma((3, coils)), dma((3,)), dma((3,)), dma((3,)), dma((2,)),
        ],
        compiler_params=pltpu.CompilerParams(
            collective_id=0, has_side_effects=True, vmem_limit_bytes=63 * 2**20),
    )(image, sensitivity, kernel.reshape(gx * kys, gz), *[jnp.asarray(t) for t in tables])


def with_halo(cells, axis, dim):
    count = lax.axis_size(axis)
    head = lax.slice_in_dim(cells, 0, 1, axis=dim)
    tail = lax.slice_in_dim(cells, cells.shape[dim] - 1, cells.shape[dim], axis=dim)
    return jnp.concatenate(
        [
            lax.ppermute(tail, axis, [(i, i + 1) for i in range(count - 1)]),
            cells,
            lax.ppermute(head, axis, [(i + 1, i) for i in range(count - 1)]),
        ],
        axis=dim,
    )


def staged(n, image, sensitivity, kernel):
    coils, _, xs, ny, nz = sensitivity.shape
    gx, kys, gz = kernel.shape
    nx, gy = n * xs, n * kys

    def table(count_out, count_in, length, sign_value):
        both = factor(count_out, count_in, length, sign_value)
        return jnp.asarray(both.reshape(2, count_out, 2, count_in).transpose(0, 2, 1, 3))

    def apply(matrix, values, pattern):
        return jnp.einsum(pattern, matrix, values, preferred_element_type=F32)

    real, imag = sensitivity[:, 0].astype(F32), sensitivity[:, 1].astype(F32)
    images = jnp.stack(
        [real * image[0] - imag * image[1], real * image[1] + imag * image[0]], axis=1).astype(BF16)
    second = apply(table(gy, ny, gy, -1.0), images, "pqkj,cqajb->cpakb").astype(BF16)
    second = lax.all_to_all(second, "slab", split_axis=3, concat_axis=2, tiled=True)
    third = apply(table(gz, nz, gz, -1.0), second, "pqkj,cqabj->cpabk").astype(BF16)
    spectrum = apply(table(gx, nx, gx, -1.0), third, "pqkj,cqjab->cpkab")
    filtered = (spectrum * kernel).astype(BF16)
    first = apply(table(nx, gx, gx, 1.0), filtered, "pqkj,cqjab->cpkab").astype(BF16)
    back = apply(table(nz, gz, gz, 1.0), first, "pqkj,cqabj->cpabk").astype(BF16)
    back = lax.all_to_all(back, "slab", split_axis=2, concat_axis=3, tiled=True)
    cells = apply(table(ny, gy, gy, 1.0), back, "pqkj,cqajb->cpakb")
    summed = jnp.stack([
        jnp.sum(real * cells[:, 0] + imag * cells[:, 1], axis=0),
        jnp.sum(real * cells[:, 1] - imag * cells[:, 0], axis=0)])
    padded = with_halo(image.astype(BF16), "slab", 1).astype(image.dtype)
    beside = padded[:, 2:] + padded[:, :-2]
    wide = jnp.pad(image, ((0, 0), (0, 0), (1, 1), (1, 1)))
    beside = beside + wide[:, :, 2:, 1:-1] + wide[:, :, :-2, 1:-1]
    beside = beside + wide[:, :, 1:-1, 2:] + wide[:, :, 1:-1, :-2]
    return summed + smooth_weight * (6.0 * image - beside)


def solution(mesh):
    n = mesh.shape["slab"]

    def local(image, sensitivity, kernel):
        tiled = sensitivity.shape[2] == 8 and kernel.shape[1] % 2 == 0 and n % PLANES == 0 and sensitivity.shape[0] == 6
        form = fused if tiled else staged
        return form(n, image, sensitivity, kernel)

    return jax.shard_map(
        local,
        mesh=mesh,
        in_specs=(
            P(None, "slab", "scan", None),
            P("scan", None, "slab", None, None),
            P(None, "slab", None),
        ),
        out_specs=P(None, "slab", "scan", None),
        check_vma=False,
    )
```
